32 devices in a mesh: grp: 8 (over y, x, core), fsdp: 4 (over z).
Axes of the slice: x: 2, y: 2, z: 4, core: 2. Of those that a mesh axis runs over, the one named last changes fastest.
Arguments:
- layer_inputs: bfloat16 [8, 2048, 2048], P('grp', 'fsdp'), may hold values from -6 to 6
- key_cotangent: bfloat16 [8, 2048, 768], P('grp', 'fsdp'), may hold values from -0.099609375 to 0.099609375
- key_weights: bfloat16 [2048, 768], P('fsdp'), may hold values from -0.125 to 0.125
- outer_momentum: float32 [2048, 768], P('fsdp'), may hold values from -0.02 to 0.02
- state_codes: int32 [8, 2048, 768], P('grp', 'fsdp'), may hold values from 0 to 255
- first_row_max: float32 [8, 2048], P('grp', 'fsdp'), may hold values from 0.1 to 2
- first_col_max: float32 [8, 768], P('grp'), may hold values from 0.1 to 2
- second_row_max: float32 [8, 2048], P('grp', 'fsdp'), may hold values from 0.1 to 4
- second_col_max: float32 [8, 768], P('grp'), may hold values from 0.1 to 4
Outputs:
- new_weights: float32 [2048, 768], P('fsdp')
- new_momentum: float32 [2048, 768], P('fsdp')
- first_state: bfloat16 [8, 2048, 768], P('grp', 'fsdp')
- second_state: bfloat16 [8, 2048, 768], P('grp', 'fsdp')
- new_first_row_max: float32 [8, 2048], P('grp', 'fsdp')
- new_first_col_max: float32 [8, 768], P('grp')
- new_second_row_max: float32 [8, 2048], P('grp', 'fsdp')
- new_second_col_max: float32 [8, 768], P('grp')
- next_keys: bfloat16 [8, 2048, 768], P('grp', 'fsdp')
The draws below stay inside these ranges and needn't reach their ends.
All inputs are finite; a program needn't handle non-finite values. Where the reference program divides by a largest or mean magnitude, that divisor is 1e-20 or more.
Results may differ from the reference program's by a relative error of at most 0.018.
Values may be sent and summed in bfloat16 or wider, within the bound.
No kernel may reach another device: no remote copies, remote signals or barrier semaphores. Data moves between devices by JAX's collectives and lax.ppermute only.
A program may use at most 64 MiB of HBM per device.

```python
import math
import jax
import jax.numpy as jnp
from jax import lax

ROWS = 2048
COLS = 768
TOK_DEV = 512
GROUPS = 8
TOK_GRP = 2048
N_GRP = 8
N_FSDP = 4


def set_ends(result, own_key, low, top_value):
    place = [jax.random.randint(jax.random.fold_in(own_key, axis), (), 0, length) for axis, length in enumerate(result.shape)]
    main_axis = result.shape.index(max(result.shape))
    beside = place[:main_axis] + [(place[main_axis] + 1) % result.shape[main_axis]] + place[main_axis + 1:]
    return result.at[tuple(place)].set(low).at[tuple(beside)].set(top_value)


def shard_levels(own_key, shape, shards, smallest, high):
    level = 1.0
    for position, shards_of in shards:
        steps = jax.random.uniform(jax.random.fold_in(jax.random.fold_in(own_key, 6), position), (shards_of,), jnp.float32, smallest / len(shards), high / len(shards))
        level = level * jnp.repeat(jnp.exp(steps), shape[position] // shards_of).reshape((-1,) + (1,) * (len(shape) - 1 - position))
    return level


def bell_draw(stream_key, shape, width, bound, cuts=(), dtype=jnp.bfloat16):
    entries = jax.random.normal(stream_key, shape, jnp.float32) * width
    if len(cuts) > 0:
        entries = shard_levels(stream_key, shape, cuts, -0.22, 0.18) * entries
    return jnp.clip(entries, min=-bound, max=bound).astype(dtype)


def setup_inputs(seed: int = 0) -> dict:
    streams_of = jax.random.split(jax.random.key(seed), 10)
    layer_inputs = bell_draw(streams_of[0], (GROUPS, TOK_GRP, ROWS), 1.0, 6.0, ((0, 8), (1, 4)))
    key_cotangent = bell_draw(streams_of[1], (GROUPS, TOK_GRP, COLS), 0.015625, 0.099609375, ((0, 8), (1, 4)))
    key_weights = bell_draw(streams_of[2], (ROWS, COLS), ROWS ** -0.5, 0.125, ((0, 4),))
    outer_momentum = bell_draw(streams_of[3], (ROWS, COLS), 0.003, 0.02, ((0, 4),), jnp.float32)
    state_codes = set_ends(jax.random.randint(streams_of[4], (GROUPS, ROWS, COLS), 0, 256), jax.random.fold_in(streams_of[4], 1), 0, 255).astype(jnp.int32)
    first_row_max = jnp.clip(jnp.exp(math.log(2.0) - 2.9957323 * jax.random.uniform(streams_of[5], (GROUPS, ROWS), jnp.float32) ** shard_levels(streams_of[5], (GROUPS, ROWS), ((0, 8), (1, 4)), -0.2, 0.2)), 0.1, 2.0)
    first_col_max = jnp.clip(jnp.exp(math.log(2.0) - 2.9957323 * jax.random.uniform(streams_of[6], (GROUPS, COLS), jnp.float32) ** shard_levels(streams_of[6], (GROUPS, COLS), ((0, 8),), -0.2, 0.2)), 0.1, 2.0)
    second_row_max = jnp.clip(jnp.exp(math.log(4.0) - 3.6888794 * jax.random.uniform(streams_of[7], (GROUPS, ROWS), jnp.float32) ** shard_levels(streams_of[7], (GROUPS, ROWS), ((0, 8), (1, 4)), -0.2, 0.2)), 0.1, 4.0)
    second_col_max = jnp.clip(jnp.exp(math.log(4.0) - 3.6888794 * jax.random.uniform(streams_of[8], (GROUPS, COLS), jnp.float32) ** shard_levels(streams_of[8], (GROUPS, COLS), ((0, 8),), -0.2, 0.2)), 0.1, 4.0)
    return dict(layer_inputs=layer_inputs, key_cotangent=key_cotangent, key_weights=key_weights, outer_momentum=outer_momentum, state_codes=state_codes, first_row_max=first_row_max, first_col_max=first_col_max, second_row_max=second_row_max, second_col_max=second_col_max)


beta_one = 0.9
beta_two = 0.95
bias_one = 1.0 - 0.9 ** 10
bias_two = 1.0 - 0.95 ** 10
adam_eps = 1e-08
inner_rate = 0.01
weight_decay = 0.1
outer_rate = 0.7
outer_beta = 0.9
stat_eps = 1e-06

def adam_moments(gradient, packed_codes, first_rows, first_cols, second_rows, second_cols):
    first_code = (packed_codes // 16).astype(jnp.float32)
    second_code = (packed_codes % 16).astype(jnp.float32)
    first_old = jnp.minimum(first_rows[:, None], first_cols[None, :]) * (first_code - 7.5) / 7.5
    second_old = jnp.minimum(second_rows[:, None], second_cols[None, :]) * ((second_code + 1.0) / 16.0) ** 2
    first_new = beta_one * first_old + (1.0 - beta_one) * gradient
    second_new = beta_two * second_old + (1.0 - beta_two) * gradient * gradient
    return (first_new, second_new)

def pseudo_step(first_new, second_new, weights_float):
    update = first_new / bias_one / (jnp.sqrt(second_new / bias_two) + adam_eps)
    return inner_rate * (update + weight_decay * weights_float)

def reference(layer_inputs, key_cotangent, key_weights, outer_momentum, state_codes, first_row_max, first_col_max, second_row_max, second_col_max):
    weights_float = key_weights.astype(jnp.float32)

    def group_step(running, inputs):
        tokens, cotangent, packed_codes, first_rows, first_cols, second_rows, second_cols = inputs
        token_blocks = tokens.reshape(N_FSDP, TOK_DEV, ROWS)
        grad_blocks = cotangent.reshape(N_FSDP, TOK_DEV, COLS)

        def add_term(accum, pair):
            partial_term = lax.dot_general(pair[0], pair[1], (((0,), (0,)), ((), ())), preferred_element_type=jnp.float32)
            rounded = lax.optimization_barrier(partial_term.astype(jnp.bfloat16))
            return (accum + rounded.astype(jnp.float32), None)
        gradient, unused = lax.scan(add_term, jnp.zeros((ROWS, COLS), jnp.float32), (token_blocks, grad_blocks))
        first_new, second_new = adam_moments(gradient, packed_codes, first_rows, first_cols, second_rows, second_cols)
        pseudo = pseudo_step(first_new, second_new, weights_float)
        first_rmax = lax.optimization_barrier(jnp.max(jnp.abs(first_new), axis=1)) + stat_eps
        first_cmax = lax.optimization_barrier(jnp.max(jnp.abs(first_new), axis=0)) + stat_eps
        second_rmax = lax.optimization_barrier(jnp.max(second_new, axis=1)) + stat_eps
        second_cmax = lax.optimization_barrier(jnp.max(second_new, axis=0)) + stat_eps
        first_state = (first_new / jnp.minimum(first_rmax[:, None], first_cmax[None, :])).astype(jnp.bfloat16)
        second_state = (second_new / jnp.minimum(second_rmax[:, None], second_cmax[None, :])).astype(jnp.bfloat16)
        return (running + pseudo, (first_state, second_state, first_rmax, first_cmax, second_rmax, second_cmax))
    running, results = lax.scan(group_step, jnp.zeros((ROWS, COLS), jnp.float32), (layer_inputs, key_cotangent, state_codes, first_row_max, first_col_max, second_row_max, second_col_max))
    averaged = running / N_GRP
    new_momentum = outer_beta * outer_momentum + averaged
    new_weights = weights_float - outer_rate * (averaged + outer_beta * new_momentum)
    weights_half = new_weights.astype(jnp.bfloat16)

    def project(tokens):
        return jnp.dot(tokens, weights_half, preferred_element_type=jnp.float32).astype(jnp.bfloat16)
    next_keys = lax.map(project, layer_inputs)
    first_state, second_state, first_rmax, first_cmax, second_rmax, second_cmax = results
    return (new_weights, new_momentum, first_state, second_state, first_rmax, first_cmax, second_rmax, second_cmax, next_keys)
```

```python
import jax
import jax.numpy as jnp
from jax import lax
from jax.sharding import PartitionSpec as P

beta_one = 0.9
beta_two = 0.95
bias_one = 1.0 - 0.9**10
bias_two = 1.0 - 0.95**10
adam_eps = 1e-08
inner_rate = 0.01
weight_decay = 0.1
outer_rate = 0.7
outer_beta = 0.9
stat_eps = 1e-06

half_type = jnp.bfloat16


def swap(value, axis, bit):
    count = lax.axis_size(axis)
    return lax.ppermute(value, axis, [(i, i ^ bit) for i in range(count)])


def pick(value, index, dim=0):
    return lax.dynamic_index_in_dim(value, index, dim, keepdims=False)


def bits_of(count):
    return [1 << i for i in range(count.bit_length() - 1)]


def wide(value):
    return value.astype(jnp.float32)


def chunks_of(cols):
    unit = 128
    parts = cols // unit
    if cols % unit or parts < 3:
        return [(0, cols)]
    last = max(1, parts // 6)
    middle = max(1, parts // 3)
    first = parts - last - middle
    edges = [0, first * unit, (first + middle) * unit, cols]
    return list(zip(edges[:-1], edges[1:]))


def reduce_rows(partial, rows):
    count = lax.axis_size("fsdp")
    place = lax.axis_index("fsdp")
    width = partial.shape[-1]
    kept = partial.reshape(count, rows, width)
    for bit in bits_of(count):
        mine = (place // bit) % 2
        pairs = kept.reshape(kept.shape[0] // 2, 2, rows, width)
        sent = pick(pairs, 1 - mine, 1).astype(half_type)
        kept = wide(pick(pairs, mine, 1)) + wide(swap(sent, "fsdp", bit))
    return kept.reshape(rows, width)


def local(
    layer_inputs,
    key_cotangent,
    key_weights,
    outer_momentum,
    state_codes,
    first_row_max,
    first_col_max,
    second_row_max,
    second_col_max,
):
    tokens = layer_inputs[0]
    cotangent = key_cotangent[0]
    features, cols = tokens.shape[1], cotangent.shape[1]
    fsdp_count, group_count = lax.axis_size("fsdp"), lax.axis_size("grp")
    fsdp_place, group_place = lax.axis_index("fsdp"), lax.axis_index("grp")
    rows = features // fsdp_count
    split = 2 if rows % 256 == 0 and group_count % 2 == 0 else 1
    part = rows // split
    core = group_place % split

    packed_codes = state_codes[0]
    first_code = (packed_codes // 16).astype(jnp.float32)
    second_code = (packed_codes % 16).astype(jnp.float32)
    first_old = (
        jnp.minimum(first_row_max[0][:, None], first_col_max[0][None, :]) * (first_code - 7.5) / 7.5
    )
    second_old = (
        jnp.minimum(second_row_max[0][:, None], second_col_max[0][None, :])
        * ((second_code + 1.0) / 16.0) ** 2
    )
    weights_float = key_weights.astype(jnp.float32)

    firsts, seconds, averages, keys = [], [], [], []
    for low, high in chunks_of(cols):
        width = high - low
        partial = lax.dot_general(
            tokens, cotangent[:, low:high], (((0,), (0,)), ((), ())), preferred_element_type=jnp.float32
        )
        gradient = reduce_rows(partial, rows)
        first_new = beta_one * first_old[:, low:high] + (1.0 - beta_one) * gradient
        second_new = beta_two * second_old[:, low:high] + (1.0 - beta_two) * gradient * gradient
        update = first_new / bias_one / (jnp.sqrt(second_new / bias_two) + adam_eps)
        pseudo = (inner_rate * (update + weight_decay * weights_float[:, low:high])).astype(half_type)
        firsts.append(first_new)
        seconds.append(second_new)
        total = pseudo.reshape(split, part, width)
        if split == 2:
            total = wide(pick(total, core)) + wide(swap(pick(total, 1 - core), "grp", 1))
        else:
            total = wide(total[0])
        for bit in bits_of(group_count):
            if bit < split:
                continue
            total = total.astype(half_type)
            total = wide(total) + wide(swap(total, "grp", bit))
        averaged = (total / group_count).astype(half_type)
        own_weights = pick(weights_float[:, low:high].reshape(split, part, width), core)
        own_momentum = pick(outer_momentum[:, low:high].reshape(split, part, width), core)
        momentum = outer_beta * own_momentum + wide(averaged)
        stepped = own_weights - outer_rate * (wide(averaged) + outer_beta * momentum)
        gathered = stepped.astype(half_type)[None]
        order = [0]
        for bit in reversed(bits_of(fsdp_count)):
            gathered = jnp.concatenate([gathered, swap(gathered, "fsdp", bit)])
            order = order + [o ^ bit for o in order]
        if split == 2:
            packed = jnp.concatenate([gathered, averaged[None]])
            other = swap(packed, "grp", 1)
            halves = jnp.stack([packed, other])
            halves = jnp.stack([pick(halves, core), pick(halves, 1 - core)], 1)
        else:
            halves = jnp.concatenate([gathered, averaged[None]])[:, None]
        averages.append(halves[fsdp_count].reshape(rows, width))
        blocks = halves[:fsdp_count].reshape(fsdp_count, rows, width)
        slot = {o: i for i, o in enumerate(order)}
        table = jnp.asarray([slot[o] for o in range(fsdp_count)], jnp.int32)
        weights_half = jnp.concatenate([pick(blocks, table[fsdp_place ^ d]) for d in range(fsdp_count)])
        keys.append(jnp.dot(tokens, weights_half, preferred_element_type=jnp.float32).astype(half_type))

    first_new = jnp.concatenate(firsts, 1)
    second_new = jnp.concatenate(seconds, 1)
    averaged = wide(jnp.concatenate(averages, 1))
    next_keys = jnp.concatenate(keys, 1)
    first_rmax = jnp.max(jnp.abs(first_new), axis=1) + stat_eps
    second_rmax = jnp.max(second_new, axis=1) + stat_eps
    both = jnp.stack([jnp.max(jnp.abs(first_new), axis=0), jnp.max(second_new, axis=0)])
    for bit in bits_of(fsdp_count):
        both = jnp.maximum(both, swap(both, "fsdp", bit))
    first_cmax = both[0] + stat_eps
    second_cmax = both[1] + stat_eps
    first_state = (first_new / jnp.minimum(first_rmax[:, None], first_cmax[None, :])).astype(half_type)
    second_state = (second_new / jnp.minimum(second_rmax[:, None], second_cmax[None, :])).astype(half_type)
    momentum = outer_beta * outer_momentum + averaged
    new_weights = weights_float - outer_rate * (averaged + outer_beta * momentum)
    return (
        new_weights,
        momentum,
        first_state[None],
        second_state[None],
        first_rmax[None],
        first_cmax[None],
        second_rmax[None],
        second_cmax[None],
        next_keys[None],
    )


def solution(mesh):
    return jax.shard_map(
        local,
        mesh=mesh,
        in_specs=(
            P("grp", "fsdp", None),
            P("grp", "fsdp", None),
            P("fsdp", None),
            P("fsdp", None),
            P("grp", "fsdp", None),
            P("grp", "fsdp"),
            P("grp", None),
            P("grp", "fsdp"),
            P("grp", None),
        ),
        out_specs=(
            P("fsdp", None),
            P("fsdp", None),
            P("grp", "fsdp", None),
            P("grp", "fsdp", None),
            P("grp", "fsdp"),
            P("grp", None),
            P("grp", "fsdp"),
            P("grp", None),
            P("grp", "fsdp", None),
        ),
        check_vma=False,
    )
```
